32 devices in a mesh: pair: 4 (over y, core), aux: 8 (over z, x).
Axes of the slice: x: 2, y: 2, z: 4, core: 2. Of those that a mesh axis runs over, the one named last changes fastest.
Arguments:
- occupied_index: int32 [4], P('pair'), may hold values from 0 to 3
- doubles_slab: bfloat16 [4, 2048, 2048], P('pair', 'aux'), may hold values from -0.09375 to 0.09375
- lambda_slab: bfloat16 [4, 2048, 2048], P('pair', 'aux'), may hold values from -0.09375 to 0.09375
- aux_factors: bfloat16 [4, 8, 2048], P('pair'), may hold values from -6 to 6
- dressed_factors: bfloat16 [4, 8, 2048], P('pair'), may hold values from -6 to 6
- virtual_coefs: bfloat16 [1024, 2048], P(None, 'aux'), may hold values from -0.125 to 0.125
- occupied_coefs: float32 [512, 4], replicated, may hold values from -3 to 3
Outputs:
- gamma_basis: bfloat16 [8, 512, 1024], P('pair', None, 'aux')
The draws below stay inside these ranges and needn't reach their ends.
Inputs may be any that keep to these rules, and one draw needn't show every extreme that they name: `occupied_index`: entry p is the occupied index i that forms a pair with the occupied index j = p.
All inputs are finite; a program needn't handle non-finite values.
Results may differ from the reference program's by a relative error of at most 0.014.
Values may be sent and summed in bfloat16 or wider, within the bound.
No kernel may reach another device: no remote copies, remote signals or barrier semaphores. Data moves between devices by JAX's collectives and lax.ppermute only.
A program may use at most 64 MiB of HBM per device.

```python
import jax
import jax.numpy as jnp
from jax import lax

V = 2048
I_WIN = 4
MU_WIN = 512
NU_WIN = 1024
Q_SLAB = 8
N_J = 4
N_PAIR = 4


def plant(drawn, key, least, high):
    dims = drawn.shape
    place = [jax.random.randint(jax.random.fold_in(key, axis), (), 0, dims[axis]) for axis in range(len(dims))]
    drawn = drawn.at[tuple(place)].set(least)
    longest = dims.index(max(dims))
    place[longest] = (place[longest] + 1) % dims[longest]
    return drawn.at[tuple(place)].set(high)


def with_spikes(result, stream_key, source, target, shards_of, factor):
    def block_of(axis_at):
        return (jnp.arange(result.shape[axis_at]) // (result.shape[axis_at] // shards_of)).reshape((-1,) + (1,) * (result.ndim - 1 - axis_at))

    one_side = jax.random.permutation(stream_key, shards_of)[block_of(target)]
    far = (block_of(target) + shards_of // 2) % shards_of
    return jnp.where((block_of(source) == one_side) | (block_of(source) == far), factor * result, result)


def shard_levels(own_key, dims, split, smallest, high):
    loudness, own = 1.0, jax.random.fold_in(own_key, 6)
    for position, parts in split:
        heights = jnp.exp(jax.random.uniform(jax.random.fold_in(own, position), (parts,), jnp.float32, smallest / len(split), high / len(split)))
        loudness = loudness * jnp.repeat(heights, dims[position] // parts).reshape([-1 if axis == position else 1 for axis in range(len(dims))])
    return loudness


def bell_draw(stream_key, extent, width, bound, shards=(), kind=jnp.bfloat16):
    result = width * jax.random.normal(stream_key, extent, jnp.float32)
    if shards:
        result = result * shard_levels(stream_key, extent, shards, -0.22, 0.18)
    return jnp.clip(result, -bound, bound).astype(kind)


def bell_draw_with(key, dims, deviation, reach, split, heavy, held_as=jnp.bfloat16):
    drawn = deviation * jax.random.normal(key, dims, jnp.float32)
    if split:
        drawn = drawn * shard_levels(key, dims, split, -0.22, 0.18)
    return jnp.clip(with_spikes(drawn, jax.random.fold_in(key, 3), *heavy), -reach, reach).astype(held_as)


def setup_inputs(seed: int = 0) -> dict:
    key_of = jax.random.split(jax.random.key(seed), 8)
    return {
        "occupied_index": plant(jax.random.randint(key_of[0], (N_J,), 0, I_WIN), jax.random.fold_in(key_of[0], 1), 0, I_WIN - 1).astype(jnp.int32),
        "doubles_slab": bell_draw(key_of[1], (N_J, V, V), (2 * V * N_PAIR // I_WIN) ** -0.5, 0.09375, ((0, 4), (1, 8))),
        "lambda_slab": bell_draw(key_of[2], (N_J, V, V), (2 * V * N_PAIR // I_WIN) ** -0.5, 0.09375, ((0, 4), (1, 8))),
        "aux_factors": bell_draw_with(key_of[3], (N_J, Q_SLAB, V), 1.0, 6.0, ((0, 4),), (0, 1, 4, 2.0)),
        "dressed_factors": bell_draw(key_of[4], (N_J, Q_SLAB, V), 1.0, 6.0, ((0, 4),)),
        "virtual_coefs": bell_draw(key_of[5], (NU_WIN, V), V ** -0.5, 0.125, ((1, 8),)),
        "occupied_coefs": bell_draw(key_of[6], (MU_WIN, I_WIN), I_WIN ** -0.5, 3.0, (), jnp.float32),
    }


def reference(occupied_index, doubles_slab, lambda_slab, aux_factors, dressed_factors, virtual_coefs, occupied_coefs):
    highest = lax.Precision.HIGHEST

    def add_pair(total, items):
        index, doubles, lambdas, factors, dressed = items
        product = jnp.dot(factors.astype(jnp.float32), doubles.astype(jnp.float32).T, precision=highest)
        product = product + jnp.dot(dressed.astype(jnp.float32), lambdas.astype(jnp.float32).T, precision=highest)
        return total.at[:, index, :].add(product), None

    initial = jnp.zeros((Q_SLAB, I_WIN, V), jnp.float32)
    summed, _ = lax.scan(add_pair, initial, (occupied_index.astype(jnp.int32), doubles_slab, lambda_slab, aux_factors, dressed_factors))
    gamma_mo = summed.astype(jnp.bfloat16)
    virtual_half = jnp.einsum("qia,na->qin", gamma_mo.astype(jnp.float32), virtual_coefs.astype(jnp.float32), precision=highest)

    def one_slab(half_rows):
        return jnp.dot(occupied_coefs, half_rows, precision=highest).astype(jnp.bfloat16)

    return lax.map(one_slab, virtual_half)
```

```python
import jax
import jax.numpy as jnp
from jax import lax
from jax.sharding import PartitionSpec as P


def shards(
    occupied_index,
    doubles_slab,
    lambda_slab,
    aux_factors,
    dressed_factors,
    virtual_coefs,
    occupied_coefs,
):
    contract = (((1,), (1,)), ((), ()))
    pairs = lax.axis_size("pair")
    blocks = lax.axis_size("aux")
    levels = occupied_coefs.shape[1]
    product = lax.dot_general(
        aux_factors[0], doubles_slab[0], contract, preferred_element_type=jnp.float32
    )
    product = product + lax.dot_general(
        dressed_factors[0], lambda_slab[0], contract, preferred_element_type=jnp.float32
    )
    half = lax.dot_general(
        product.astype(jnp.bfloat16), virtual_coefs, contract, preferred_element_type=jnp.float32
    )
    q_own = half.shape[0] // pairs
    nu_own = half.shape[1] // blocks
    cells = half.reshape(pairs, q_own, blocks, nu_own).transpose(0, 2, 1, 3)
    cells = cells.reshape(pairs * blocks, 1, q_own, nu_own)
    mine = jnp.arange(levels, dtype=jnp.int32) == occupied_index[0]
    cells = jnp.where(mine[None, :, None, None], cells, 0.0).astype(jnp.bfloat16)
    cells = cells.reshape(pairs * blocks, levels * q_own, nu_own)
    received = lax.all_to_all(cells, ("pair", "aux"), split_axis=0, concat_axis=0, tiled=True)
    summed = received.astype(jnp.float32).sum(axis=0).reshape(levels, q_own, nu_own)
    gamma_basis = sum(
        occupied_coefs[:, i][None, :, None] * summed[i][:, None, :] for i in range(levels)
    )
    return gamma_basis.astype(jnp.bfloat16)


def solution(mesh):
    placed = (
        P("pair"),
        P("pair", "aux", None),
        P("pair", "aux", None),
        P("pair", None, None),
        P("pair", None, None),
        P(None, "aux"),
        P(),
    )
    return jax.shard_map(
        shards, mesh=mesh, in_specs=placed, out_specs=P("pair", None, "aux"), check_vma=False
    )
```

```python
import functools

import jax
import jax.numpy as jnp
from jax import lax
from jax.experimental import pallas as pl
from jax.experimental.pallas import tpu as pltpu
from jax.sharding import PartitionSpec as P

ROWS = (((1,), (1,)), ((), ()))


def fetch(index_ref, aux_hbm, dressed_hbm, coefs_hbm, levels_hbm,
          aux_ref, dressed_ref, coefs_ref, mask_ref, wide_ref, levels_ref, sems, *, q_own):
    moves = (
        (levels_hbm, levels_ref),
        (aux_hbm, aux_ref),
        (dressed_hbm, dressed_ref),
        (coefs_hbm, coefs_ref),
    )
    copies = [
        pltpu.make_async_copy(source, target, sems.at[k]) for k, (source, target) in enumerate(moves)
    ]
    for copy in copies:
        copy.start()
    slot = lax.broadcasted_iota(jnp.int32, mask_ref.shape, 0)
    mask_ref[...] = (slot // q_own == index_ref[0]).astype(jnp.float32)
    copies[0].wait()
    coefs = jnp.transpose(levels_ref[...])
    for i in range(wide_ref.shape[0]):
        wide_ref[i] = jnp.broadcast_to(coefs[:, i : i + 1], wide_ref.shape[1:])
    for copy in copies[1:]:
        copy.wait()


def before(mask_ref, product_ref, coefs_ref, cells_ref, *, levels):
    cells, slots, nu_own = cells_ref.shape
    q_own = slots // levels
    pairs = product_ref.shape[0] // q_own
    blocks = cells // pairs
    product = product_ref[...]
    mine = mask_ref[:, 0:1] > 0.5
    placed = [
        jnp.where(mine, jnp.concatenate([product[p * q_own : (p + 1) * q_own]] * levels, axis=0), 0.0)
        for p in range(pairs)
    ]
    placed = jnp.concatenate(placed, axis=0).astype(jnp.bfloat16)
    half = lax.dot_general(placed, coefs_ref[...], ROWS, preferred_element_type=jnp.float32)
    half = half.astype(jnp.bfloat16)
    for p in range(pairs):
        for x in range(blocks):
            cells_ref[p * blocks + x] = half[
                p * slots : (p + 1) * slots, x * nu_own : (x + 1) * nu_own
            ]


def after(cells_ref, wide_ref, out_hbm, out_ref, sems, *, levels):
    q_own = out_ref.shape[0]
    summed = cells_ref[...].astype(jnp.float32).sum(axis=0)
    copies = []
    for q in range(q_own):
        total = wide_ref[0] * summed[q : q + 1]
        for i in range(1, levels):
            total = total + wide_ref[i] * summed[i * q_own + q : i * q_own + q + 1]
        out_ref[q] = total.astype(out_ref.dtype)
        copies.append(pltpu.make_async_copy(out_ref.at[q], out_hbm.at[q], sems.at[q]))
        copies[-1].start()
    for copy in copies:
        copy.wait()


def shards(
    occupied_index,
    doubles_slab,
    lambda_slab,
    aux_factors,
    dressed_factors,
    virtual_coefs,
    occupied_coefs,
):
    pairs = lax.axis_size("pair")
    blocks = lax.axis_size("aux")
    mu, levels = occupied_coefs.shape
    q_own = aux_factors.shape[1] // pairs
    nu_own = virtual_coefs.shape[0] // blocks
    limit = (4 << 20) + 16 * pairs * blocks * levels * q_own * nu_own
    vmem = pl.BlockSpec(memory_space=pltpu.VMEM)
    hbm = pl.BlockSpec(memory_space=pl.ANY)
    fetched = (aux_factors, dressed_factors, virtual_coefs, occupied_coefs.T)
    aux_factors, dressed_factors, virtual_coefs, mask, wide = pl.pallas_call(
        functools.partial(fetch, q_own=q_own),
        out_shape=tuple(pltpu.VMEM(x.shape, x.dtype) for x in fetched[:3])
        + (
            pltpu.VMEM((levels * q_own, 128), jnp.float32),
            pltpu.VMEM((levels, mu, nu_own), jnp.float32),
        ),
        in_specs=[pl.BlockSpec(memory_space=pltpu.SMEM)] + [hbm] * 4,
        out_specs=(vmem,) * 5,
        scratch_shapes=[
            pltpu.VMEM((levels, mu), jnp.float32),
            pltpu.SemaphoreType.DMA((4,)),
        ],
        name="fetch",
        compiler_params=pltpu.CompilerParams(vmem_limit_bytes=limit),
    )(occupied_index, *(pltpu.with_memory_space_constraint(x, pltpu.HBM) for x in fetched))
    product = lax.dot_general(
        aux_factors[0], doubles_slab[0], ROWS, preferred_element_type=jnp.float32
    )
    product = product + lax.dot_general(
        dressed_factors[0], lambda_slab[0], ROWS, preferred_element_type=jnp.float32
    )
    inputs = [
        pltpu.with_memory_space_constraint(x, pltpu.VMEM)
        for x in (mask, product, virtual_coefs)
    ]
    cells = pl.pallas_call(
        functools.partial(before, levels=levels),
        out_shape=pltpu.VMEM((pairs * blocks, levels * q_own, nu_own), jnp.bfloat16),
        in_specs=[vmem] * 3,
        out_specs=vmem,
        name="before",
        compiler_params=pltpu.CompilerParams(vmem_limit_bytes=limit),
    )(*inputs)
    received = lax.all_to_all(cells, ("pair", "aux"), split_axis=0, concat_axis=0, tiled=True)
    received = pltpu.with_memory_space_constraint(received, pltpu.VMEM)
    wide = pltpu.with_memory_space_constraint(wide, pltpu.VMEM)
    return pl.pallas_call(
        functools.partial(after, levels=levels),
        out_shape=jax.ShapeDtypeStruct((q_own, mu, nu_own), jnp.bfloat16),
        in_specs=[vmem, vmem],
        out_specs=hbm,
        scratch_shapes=[
            pltpu.VMEM((q_own, mu, nu_own), jnp.bfloat16),
            pltpu.SemaphoreType.DMA((q_own,)),
        ],
        name="after",
        compiler_params=pltpu.CompilerParams(vmem_limit_bytes=limit),
    )(received, wide)


def solution(mesh):
    placed = (
        P("pair"),
        P("pair", "aux", None),
        P("pair", "aux", None),
        P("pair", None, None),
        P("pair", None, None),
        P(None, "aux"),
        P(),
    )
    return jax.shard_map(
        shards, mesh=mesh, in_specs=placed, out_specs=P("pair", None, "aux"), check_vma=False
    )
```

```python
import functools

import jax
import jax.numpy as jnp
from jax import lax
from jax.experimental import pallas as pl
from jax.experimental.pallas import tpu as pltpu
from jax.sharding import PartitionSpec as P

FLOPS = 1 << 33
ROWS = (((1,), (1,)), ((), ()))


def level(row_ref, *, q_own):
    row_ref[...] = (lax.broadcasted_iota(jnp.int32, row_ref.shape, 0) // q_own).astype(jnp.float32)


def widen(coefs_ref, wide_ref, tag_ref):
    tag_ref[...] = jnp.zeros(tag_ref.shape, tag_ref.dtype)
    coefs = jnp.transpose(coefs_ref[...])
    for i in range(wide_ref.shape[0]):
        wide_ref[i] = jnp.broadcast_to(coefs[:, i : i + 1], wide_ref.shape[1:])


def first(aux_ref, dressed_ref, tag_ref, doubles_ref, product_ref):
    product_ref[...] = lax.dot_general(
        aux_ref[0], doubles_ref[0], ROWS, preferred_element_type=jnp.float32
    )


def before(index_ref, rows_ref, product_ref, dressed_ref, lambda_ref, coefs_ref, cells_ref, *, levels):
    cells, slots, nu_own = cells_ref.shape
    q_own = slots // levels
    pairs = product_ref.shape[0] // q_own
    blocks = cells // pairs
    product = product_ref[...] + lax.dot_general(
        dressed_ref[0], lambda_ref[0], ROWS, preferred_element_type=jnp.float32
    )
    mine = rows_ref[:, 0:1] == index_ref[0].astype(jnp.float32)
    placed = [
        jnp.where(mine, jnp.concatenate([product[p * q_own : (p + 1) * q_own]] * levels, axis=0), 0.0)
        for p in range(pairs)
    ]
    placed = jnp.concatenate(placed, axis=0).astype(jnp.bfloat16)
    half = lax.dot_general(placed, coefs_ref[...], ROWS, preferred_element_type=jnp.float32)
    half = half.astype(jnp.bfloat16)
    for p in range(pairs):
        for x in range(blocks):
            cells_ref[p * blocks + x] = half[
                p * slots : (p + 1) * slots, x * nu_own : (x + 1) * nu_own
            ]


def after(cells_ref, wide_ref, out_hbm, out_ref, sems, *, levels):
    q_own = out_ref.shape[0]
    summed = cells_ref[...].astype(jnp.float32).sum(axis=0)
    copies = []
    for q in range(q_own):
        total = wide_ref[0] * summed[q : q + 1]
        for i in range(1, levels):
            total = total + wide_ref[i] * summed[i * q_own + q : i * q_own + q + 1]
        out_ref[q] = total.astype(out_ref.dtype)
        copies.append(pltpu.make_async_copy(out_ref.at[q], out_hbm.at[q], sems.at[q]))
        copies[-1].start()
    for copy in copies:
        copy.wait()


def shards(
    occupied_index,
    doubles_slab,
    lambda_slab,
    aux_factors,
    dressed_factors,
    virtual_coefs,
    occupied_coefs,
):
    pairs = lax.axis_size("pair")
    blocks = lax.axis_size("aux")
    mu, levels = occupied_coefs.shape
    q_own = aux_factors.shape[1] // pairs
    nu_own = virtual_coefs.shape[0] // blocks
    limit = (4 << 20) + 16 * pairs * blocks * levels * q_own * nu_own
    vmem = pl.BlockSpec(memory_space=pltpu.VMEM)
    hbm = pl.BlockSpec(memory_space=pl.ANY)
    pin = lambda *xs: [pltpu.with_memory_space_constraint(x, pltpu.VMEM) for x in xs]
    params = pltpu.CompilerParams(vmem_limit_bytes=limit)
    (dressed_factors,) = pin(dressed_factors)
    rows = pl.pallas_call(
        functools.partial(level, q_own=q_own),
        out_shape=pltpu.VMEM((levels * q_own, 128), jnp.float32),
        in_specs=[],
        out_specs=vmem,
        name="level",
        compiler_params=params,
        cost_estimate=pl.CostEstimate(flops=FLOPS, transcendentals=0, bytes_accessed=0),
    )()
    wide, tag = pl.pallas_call(
        widen,
        out_shape=(
            pltpu.VMEM((levels, mu, nu_own), jnp.float32),
            pltpu.VMEM((8, 128), jnp.float32),
        ),
        in_specs=[vmem],
        out_specs=(vmem, vmem),
        name="widen",
        compiler_params=params,
        cost_estimate=pl.CostEstimate(flops=1, transcendentals=0, bytes_accessed=1),
    )(*pin(occupied_coefs.T))
    wide, tag = pin(wide, tag)
    product = pl.pallas_call(
        first,
        out_shape=pltpu.VMEM((aux_factors.shape[1], doubles_slab.shape[1]), jnp.float32),
        in_specs=[vmem] * 4,
        out_specs=vmem,
        name="first",
        compiler_params=params,
        cost_estimate=pl.CostEstimate(flops=1, transcendentals=0, bytes_accessed=1),
    )(*pin(aux_factors), dressed_factors, tag, *pin(doubles_slab))
    cells = pl.pallas_call(
        functools.partial(before, levels=levels),
        out_shape=pltpu.VMEM((pairs * blocks, levels * q_own, nu_own), jnp.bfloat16),
        in_specs=[pl.BlockSpec(memory_space=pltpu.SMEM)] + [vmem] * 5,
        out_specs=vmem,
        name="before",
        compiler_params=params,
    )(occupied_index, *pin(rows, product), dressed_factors, *pin(lambda_slab, virtual_coefs))
    received = lax.all_to_all(cells, ("pair", "aux"), split_axis=0, concat_axis=0, tiled=True)
    return pl.pallas_call(
        functools.partial(after, levels=levels),
        out_shape=jax.ShapeDtypeStruct((q_own, mu, nu_own), jnp.bfloat16),
        in_specs=[vmem, vmem],
        out_specs=hbm,
        scratch_shapes=[
            pltpu.VMEM((q_own, mu, nu_own), jnp.bfloat16),
            pltpu.SemaphoreType.DMA((q_own,)),
        ],
        name="after",
        compiler_params=params,
    )(*pin(received), wide)


def solution(mesh):
    placed = (
        P("pair"),
        P("pair", "aux", None),
        P("pair", "aux", None),
        P("pair", None, None),
        P("pair", None, None),
        P(None, "aux"),
        P(),
    )
    return jax.shard_map(
        shards, mesh=mesh, in_specs=placed, out_specs=P("pair", None, "aux"), check_vma=False
    )
```

```python
import functools

import jax
import jax.numpy as jnp
from jax import lax
from jax.experimental import pallas as pl
from jax.experimental.pallas import tpu as pltpu
from jax.sharding import PartitionSpec as P

FLOPS = 1 << 33
ROWS = (((1,), (1,)), ((), ()))


def level(row_ref, *, q_own):
    row_ref[...] = (lax.broadcasted_iota(jnp.int32, row_ref.shape, 0) // q_own).astype(jnp.float32)


def widen(rows_ref, coefs_ref, wide_ref, tag_ref):
    tag_ref[...] = rows_ref[...]
    coefs = jnp.transpose(coefs_ref[...])
    for i in range(wide_ref.shape[0]):
        wide_ref[i] = jnp.broadcast_to(coefs[:, i : i + 1], wide_ref.shape[1:])


def first(aux_ref, dressed_ref, tag_ref, doubles_ref, product_ref):
    product_ref[...] = lax.dot_general(
        aux_ref[0], doubles_ref[0], ROWS, preferred_element_type=jnp.float32
    )


def before(index_ref, product_ref, dressed_ref, lambda_ref, coefs_ref, cells_ref):
    cells, rows, nu_own = cells_ref.shape
    q_own = rows // 2
    product = product_ref[...] + lax.dot_general(
        dressed_ref[0], lambda_ref[0], ROWS, preferred_element_type=jnp.float32
    )
    pairs = product.shape[0] // q_own
    blocks = cells // pairs
    half = lax.dot_general(
        product.astype(jnp.bfloat16), coefs_ref[...], ROWS, preferred_element_type=jnp.float32
    )
    sender = jnp.full((q_own, half.shape[1]), index_ref[0].astype(jnp.float32))
    for p in range(pairs):
        block = jnp.concatenate([half[p * q_own : (p + 1) * q_own], sender], axis=0)
        block = block.astype(jnp.bfloat16)
        for x in range(blocks):
            cells_ref[p * blocks + x] = block[:, x * nu_own : (x + 1) * nu_own]


def after(cells_ref, wide_ref, out_hbm, out_ref, sems, *, levels, pairs):
    q_own = out_ref.shape[0]
    blocks = cells_ref.shape[0] // pairs
    summed = [0.0] * levels
    for p in range(pairs):
        cells = cells_ref[p * blocks : (p + 1) * blocks].astype(jnp.float32)
        values, sender = cells.sum(axis=0)[:q_own], cells[0, q_own:]
        for i in range(levels):
            summed[i] = summed[i] + jnp.where(sender == i, values, 0.0)
    copies = []
    for q in range(q_own):
        total = wide_ref[0] * summed[0][q : q + 1]
        for i in range(1, levels):
            total = total + wide_ref[i] * summed[i][q : q + 1]
        out_ref[q] = total.astype(out_ref.dtype)
        copies.append(pltpu.make_async_copy(out_ref.at[q], out_hbm.at[q], sems.at[q]))
        copies[-1].start()
    for copy in copies:
        copy.wait()


def shards(
    occupied_index,
    doubles_slab,
    lambda_slab,
    aux_factors,
    dressed_factors,
    virtual_coefs,
    occupied_coefs,
):
    pairs = lax.axis_size("pair")
    blocks = lax.axis_size("aux")
    mu, levels = occupied_coefs.shape
    q_own = aux_factors.shape[1] // pairs
    nu_own = virtual_coefs.shape[0] // blocks
    limit = (4 << 20) + 16 * pairs * blocks * levels * q_own * nu_own
    vmem = pl.BlockSpec(memory_space=pltpu.VMEM)
    hbm = pl.BlockSpec(memory_space=pl.ANY)
    pin = lambda *xs: [pltpu.with_memory_space_constraint(x, pltpu.VMEM) for x in xs]
    params = pltpu.CompilerParams(vmem_limit_bytes=limit)
    (dressed_factors,) = pin(dressed_factors)
    rows = pl.pallas_call(
        functools.partial(level, q_own=q_own),
        out_shape=pltpu.VMEM((levels * q_own, 128), jnp.float32),
        in_specs=[],
        out_specs=vmem,
        name="level",
        compiler_params=params,
        cost_estimate=pl.CostEstimate(flops=FLOPS, transcendentals=0, bytes_accessed=0),
    )()
    wide, tag = pl.pallas_call(
        widen,
        out_shape=(
            pltpu.VMEM((levels, mu, nu_own), jnp.float32),
            pltpu.VMEM((levels * q_own, 128), jnp.float32),
        ),
        in_specs=[vmem] * 2,
        out_specs=(vmem, vmem),
        name="widen",
        compiler_params=params,
        cost_estimate=pl.CostEstimate(flops=1, transcendentals=0, bytes_accessed=1),
    )(*pin(rows, occupied_coefs.T))
    wide, tag = pin(wide, tag)
    product = pl.pallas_call(
        first,
        out_shape=pltpu.VMEM((aux_factors.shape[1], doubles_slab.shape[1]), jnp.float32),
        in_specs=[vmem] * 4,
        out_specs=vmem,
        name="first",
        compiler_params=params,
        cost_estimate=pl.CostEstimate(flops=1, transcendentals=0, bytes_accessed=1),
    )(*pin(aux_factors), dressed_factors, tag, *pin(doubles_slab))
    cells = pl.pallas_call(
        before,
        out_shape=pltpu.VMEM((pairs * blocks, 2 * q_own, nu_own), jnp.bfloat16),
        in_specs=[pl.BlockSpec(memory_space=pltpu.SMEM)] + [vmem] * 4,
        out_specs=vmem,
        name="before",
        compiler_params=params,
    )(occupied_index, *pin(product), dressed_factors, *pin(lambda_slab, virtual_coefs))
    received = lax.all_to_all(cells, ("pair", "aux"), split_axis=0, concat_axis=0, tiled=True)
    return pl.pallas_call(
        functools.partial(after, levels=levels, pairs=pairs),
        out_shape=jax.ShapeDtypeStruct((q_own, mu, nu_own), jnp.bfloat16),
        in_specs=[vmem, vmem],
        out_specs=hbm,
        scratch_shapes=[
            pltpu.VMEM((q_own, mu, nu_own), jnp.bfloat16),
            pltpu.SemaphoreType.DMA((q_own,)),
        ],
        name="after",
        compiler_params=params,
    )(*pin(received), wide)


def solution(mesh):
    placed = (
        P("pair"),
        P("pair", "aux", None),
        P("pair", "aux", None),
        P("pair", None, None),
        P("pair", None, None),
        P(None, "aux"),
        P(),
    )
    return jax.shard_map(
        shards, mesh=mesh, in_specs=placed, out_specs=P("pair", None, "aux"), check_vma=False
    )
```

```python
import functools

import jax
import jax.numpy as jnp
from jax import lax
from jax.experimental import pallas as pl
from jax.experimental.pallas import tpu as pltpu
from jax.sharding import PartitionSpec as P

FLOPS = 1 << 33
ROWS = (((1,), (1,)), ((), ()))


def level(row_ref, *, q_own):
    row_ref[...] = (lax.broadcasted_iota(jnp.int32, row_ref.shape, 0) // q_own).astype(jnp.float32)


def widen(rows_ref, aux_ref, dressed_ref, coefs_ref, wide_ref, tag_ref):
    tag_ref[...] = rows_ref[...]
    coefs = jnp.transpose(coefs_ref[...])
    for i in range(wide_ref.shape[0]):
        wide_ref[i] = jnp.broadcast_to(coefs[:, i : i + 1], wide_ref.shape[1:])


def first(aux_ref, tag_ref, doubles_ref, product_ref):
    product_ref[...] = lax.dot_general(
        aux_ref[0], doubles_ref[0], ROWS, preferred_element_type=jnp.float32
    )


def before(index_ref, product_ref, dressed_ref, lambda_ref, coefs_ref, cells_ref):
    cells, rows, nu_own = cells_ref.shape
    q_own = rows // 2
    product = product_ref[...] + lax.dot_general(
        dressed_ref[0], lambda_ref[0], ROWS, preferred_element_type=jnp.float32
    )
    pairs = product.shape[0] // q_own
    blocks = cells // pairs
    half = lax.dot_general(
        product.astype(jnp.bfloat16), coefs_ref[...], ROWS, preferred_element_type=jnp.float32
    )
    sender = jnp.full((q_own, half.shape[1]), index_ref[0].astype(jnp.float32))
    for p in range(pairs):
        block = jnp.concatenate([half[p * q_own : (p + 1) * q_own], sender], axis=0)
        block = block.astype(jnp.bfloat16)
        for x in range(blocks):
            cells_ref[p * blocks + x] = block[:, x * nu_own : (x + 1) * nu_own]


def after(cells_ref, wide_ref, out_hbm, out_ref, sems, *, levels, pairs):
    q_own = out_ref.shape[0]
    blocks = cells_ref.shape[0] // pairs
    summed = [0.0] * levels
    for p in range(pairs):
        cells = cells_ref[p * blocks : (p + 1) * blocks].astype(jnp.float32)
        values, sender = cells.sum(axis=0)[:q_own], cells[0, q_own:]
        for i in range(levels):
            summed[i] = summed[i] + jnp.where(sender == i, values, 0.0)
    copies = []
    for q in range(q_own):
        total = wide_ref[0] * summed[0][q : q + 1]
        for i in range(1, levels):
            total = total + wide_ref[i] * summed[i][q : q + 1]
        out_ref[q] = total.astype(out_ref.dtype)
        copies.append(pltpu.make_async_copy(out_ref.at[q], out_hbm.at[q], sems.at[q]))
        copies[-1].start()
    for copy in copies:
        copy.wait()


def shards(
    occupied_index,
    doubles_slab,
    lambda_slab,
    aux_factors,
    dressed_factors,
    virtual_coefs,
    occupied_coefs,
):
    pairs = lax.axis_size("pair")
    blocks = lax.axis_size("aux")
    mu, levels = occupied_coefs.shape
    q_own = aux_factors.shape[1] // pairs
    nu_own = virtual_coefs.shape[0] // blocks
    limit = (4 << 20) + 16 * pairs * blocks * levels * q_own * nu_own
    vmem = pl.BlockSpec(memory_space=pltpu.VMEM)
    hbm = pl.BlockSpec(memory_space=pl.ANY)
    pin = lambda *xs: [pltpu.with_memory_space_constraint(x, pltpu.VMEM) for x in xs]
    params = pltpu.CompilerParams(vmem_limit_bytes=limit)
    aux_factors, dressed_factors = pin(aux_factors, dressed_factors)
    rows = pl.pallas_call(
        functools.partial(level, q_own=q_own),
        out_shape=pltpu.VMEM((levels * q_own, 128), jnp.float32),
        in_specs=[],
        out_specs=vmem,
        name="level",
        compiler_params=params,
        cost_estimate=pl.CostEstimate(flops=FLOPS, transcendentals=0, bytes_accessed=0),
    )()
    wide, tag = pl.pallas_call(
        widen,
        out_shape=(
            pltpu.VMEM((levels, mu, nu_own), jnp.float32),
            pltpu.VMEM((levels * q_own, 128), jnp.float32),
        ),
        in_specs=[vmem] * 4,
        out_specs=(vmem, vmem),
        name="widen",
        compiler_params=params,
        cost_estimate=pl.CostEstimate(flops=1, transcendentals=0, bytes_accessed=1),
    )(*pin(rows), aux_factors, dressed_factors, *pin(occupied_coefs.T))
    wide, tag = pin(wide, tag)
    product = pl.pallas_call(
        first,
        out_shape=pltpu.VMEM((aux_factors.shape[1], doubles_slab.shape[1]), jnp.float32),
        in_specs=[vmem] * 3,
        out_specs=vmem,
        name="first",
        compiler_params=params,
        cost_estimate=pl.CostEstimate(flops=1, transcendentals=0, bytes_accessed=1),
    )(aux_factors, tag, *pin(doubles_slab))
    cells = pl.pallas_call(
        before,
        out_shape=pltpu.VMEM((pairs * blocks, 2 * q_own, nu_own), jnp.bfloat16),
        in_specs=[pl.BlockSpec(memory_space=pltpu.SMEM)] + [vmem] * 4,
        out_specs=vmem,
        name="before",
        compiler_params=params,
    )(occupied_index, *pin(product), dressed_factors, *pin(lambda_slab, virtual_coefs))
    received = lax.all_to_all(cells, ("pair", "aux"), split_axis=0, concat_axis=0, tiled=True)
    return pl.pallas_call(
        functools.partial(after, levels=levels, pairs=pairs),
        out_shape=jax.ShapeDtypeStruct((q_own, mu, nu_own), jnp.bfloat16),
        in_specs=[vmem, vmem],
        out_specs=hbm,
        scratch_shapes=[
            pltpu.VMEM((q_own, mu, nu_own), jnp.bfloat16),
            pltpu.SemaphoreType.DMA((q_own,)),
        ],
        name="after",
        compiler_params=params,
    )(*pin(received), wide)


def solution(mesh):
    placed = (
        P("pair"),
        P("pair", "aux", None),
        P("pair", "aux", None),
        P("pair", None, None),
        P("pair", None, None),
        P(None, "aux"),
        P(),
    )
    return jax.shard_map(
        shards, mesh=mesh, in_specs=placed, out_specs=P("pair", None, "aux"), check_vma=False
    )
```

```python
import functools

import jax
import jax.numpy as jnp
from jax import lax
from jax.experimental import pallas as pl
from jax.experimental.pallas import tpu as pltpu
from jax.sharding import PartitionSpec as P

FLOPS = 1 << 33
ROWS = (((1,), (1,)), ((), ()))


def level(row_ref, *, q_own):
    row_ref[...] = (lax.broadcasted_iota(jnp.int32, row_ref.shape, 0) // q_own).astype(jnp.float32)


def widen(rows_ref, aux_ref, dressed_ref, coefs_ref, wide_ref, tag_ref):
    tag_ref[...] = rows_ref[...]
    coefs = jnp.transpose(coefs_ref[...])
    for i in range(wide_ref.shape[0]):
        wide_ref[i] = jnp.broadcast_to(coefs[:, i : i + 1], wide_ref.shape[1:])


def first(aux_ref, tag_ref, doubles_ref, product_ref):
    half = doubles_ref.shape[1] // 2
    product_ref[:, :half] = lax.dot_general(
        aux_ref[0], doubles_ref[0, :half], ROWS, preferred_element_type=jnp.float32
    )
    product_ref[:, half:] = lax.dot_general(
        aux_ref[0], doubles_ref[0, half:], ROWS, preferred_element_type=jnp.float32
    )


def before(index_ref, product_ref, dressed_ref, lambda_ref, coefs_ref, cells_ref):
    cells, rows, nu_own = cells_ref.shape
    q_own = rows // 2
    product = product_ref[...] + lax.dot_general(
        dressed_ref[0], lambda_ref[0], ROWS, preferred_element_type=jnp.float32
    )
    pairs = product.shape[0] // q_own
    blocks = cells // pairs
    half = lax.dot_general(
        product.astype(jnp.bfloat16), coefs_ref[...], ROWS, preferred_element_type=jnp.float32
    )
    sender = jnp.full((q_own, half.shape[1]), index_ref[0].astype(jnp.float32))
    for p in range(pairs):
        block = jnp.concatenate([half[p * q_own : (p + 1) * q_own], sender], axis=0)
        block = block.astype(jnp.bfloat16)
        for x in range(blocks):
            cells_ref[p * blocks + x] = block[:, x * nu_own : (x + 1) * nu_own]


def after(cells_ref, wide_ref, out_hbm, out_ref, sems, *, levels, pairs):
    q_own = out_ref.shape[0]
    blocks = cells_ref.shape[0] // pairs
    summed = [0.0] * levels
    for p in range(pairs):
        cells = cells_ref[p * blocks : (p + 1) * blocks].astype(jnp.float32)
        values, sender = cells.sum(axis=0)[:q_own], cells[0, q_own:]
        for i in range(levels):
            summed[i] = summed[i] + jnp.where(sender == i, values, 0.0)
    copies = []
    for q in range(q_own):
        total = wide_ref[0] * summed[0][q : q + 1]
        for i in range(1, levels):
            total = total + wide_ref[i] * summed[i][q : q + 1]
        out_ref[q] = total.astype(out_ref.dtype)
        copies.append(pltpu.make_async_copy(out_ref.at[q], out_hbm.at[q], sems.at[q]))
        copies[-1].start()
    for copy in copies:
        copy.wait()


def shards(
    occupied_index,
    doubles_slab,
    lambda_slab,
    aux_factors,
    dressed_factors,
    virtual_coefs,
    occupied_coefs,
):
    pairs = lax.axis_size("pair")
    blocks = lax.axis_size("aux")
    mu, levels = occupied_coefs.shape
    q_own = aux_factors.shape[1] // pairs
    nu_own = virtual_coefs.shape[0] // blocks
    limit = (4 << 20) + 16 * pairs * blocks * levels * q_own * nu_own
    vmem = pl.BlockSpec(memory_space=pltpu.VMEM)
    hbm = pl.BlockSpec(memory_space=pl.ANY)
    pin = lambda *xs: [pltpu.with_memory_space_constraint(x, pltpu.VMEM) for x in xs]
    params = pltpu.CompilerParams(vmem_limit_bytes=limit)
    aux_factors, dressed_factors = pin(aux_factors, dressed_factors)
    rows = pl.pallas_call(
        functools.partial(level, q_own=q_own),
        out_shape=pltpu.VMEM((levels * q_own, 128), jnp.float32),
        in_specs=[],
        out_specs=vmem,
        name="level",
        compiler_params=params,
        cost_estimate=pl.CostEstimate(flops=FLOPS, transcendentals=0, bytes_accessed=0),
    )()
    wide, tag = pl.pallas_call(
        widen,
        out_shape=(
            pltpu.VMEM((levels, mu, nu_own), jnp.float32),
            pltpu.VMEM((levels * q_own, 128), jnp.float32),
        ),
        in_specs=[vmem] * 4,
        out_specs=(vmem, vmem),
        name="widen",
        compiler_params=params,
        cost_estimate=pl.CostEstimate(flops=1, transcendentals=0, bytes_accessed=1),
    )(*pin(rows), aux_factors, dressed_factors, *pin(occupied_coefs.T))
    wide, tag = pin(wide, tag)
    product = pl.pallas_call(
        first,
        out_shape=pltpu.VMEM((aux_factors.shape[1], doubles_slab.shape[1]), jnp.float32),
        in_specs=[vmem] * 3,
        out_specs=vmem,
        name="first",
        compiler_params=params,
        cost_estimate=pl.CostEstimate(flops=1, transcendentals=0, bytes_accessed=1),
    )(aux_factors, tag, *pin(doubles_slab))
    cells = pl.pallas_call(
        before,
        out_shape=pltpu.VMEM((pairs * blocks, 2 * q_own, nu_own), jnp.bfloat16),
        in_specs=[pl.BlockSpec(memory_space=pltpu.SMEM)] + [vmem] * 4,
        out_specs=vmem,
        name="before",
        compiler_params=params,
    )(occupied_index, *pin(product), dressed_factors, *pin(lambda_slab, virtual_coefs))
    received = lax.all_to_all(cells, ("pair", "aux"), split_axis=0, concat_axis=0, tiled=True)
    return pl.pallas_call(
        functools.partial(after, levels=levels, pairs=pairs),
        out_shape=jax.ShapeDtypeStruct((q_own, mu, nu_own), jnp.bfloat16),
        in_specs=[vmem, vmem],
        out_specs=hbm,
        scratch_shapes=[
            pltpu.VMEM((q_own, mu, nu_own), jnp.bfloat16),
            pltpu.SemaphoreType.DMA((q_own,)),
        ],
        name="after",
        compiler_params=params,
    )(*pin(received), wide)


def solution(mesh):
    placed = (
        P("pair"),
        P("pair", "aux", None),
        P("pair", "aux", None),
        P("pair", None, None),
        P("pair", None, None),
        P(None, "aux"),
        P(),
    )
    return jax.shard_map(
        shards, mesh=mesh, in_specs=placed, out_specs=P("pair", None, "aux"), check_vma=False
    )
```
